256 devices in a mesh: col: 128 (over y, x, z), row: 2 (over core).
Axes of the slice: x: 4, y: 4, z: 8, core: 2. Of those that a mesh axis runs over, the one named last changes fastest.
Arguments:
- top_rows: float32 [1792, 65536], P(None, ('col', 'row')), may hold values from -0.0234375 to 0.0234375
- lower_new: float32 [65536, 256], P(('col', 'row')), may hold values from -6 to 6
- block_order: int32 [256, 2], P(('col', 'row')), may hold values from 0 to 1, each once within a row
- corner: float32 [1792, 1792], P('row'), may hold values from -0.125 to 0.125
- target: float32 [1792, 256], P('row'), may hold values from -6 to 6
- coupling: float32 [128, 128], replicated, may hold values from -0.5 to 0.5
- top_right: float32 [14, 128, 128], P('row'), may hold values from -0.5 to 0.5
- top_left: float32 [14, 128, 128], P('row'), may hold values from -0.5 to 0.5
- top_values: float32 [14, 128], P('row'), may hold values from 0.5 to 2
- new_right: float32 [2, 128, 128], replicated, may hold values from -0.5 to 0.5
- new_left: float32 [2, 128, 128], replicated, may hold values from -0.5 to 0.5
- new_values: float32 [2, 128], replicated, may hold values from 0.5 to 2
Outputs:
- solution: float32 [1792, 256], P('row')
The draws below stay inside these ranges and needn't reach their ends.
Inputs may be any that keep to these rules, and one draw needn't show every extreme that they name: Each row of block_order is an ordering of 0 to 1.
All inputs are finite; a program needn't handle non-finite values.
Results may differ from the reference program's by a relative error of at most 0.0001.
Values sent between devices are 32-bit elements; how exact they have to be, the bound alone decides.
A program may use at most 64 MiB of HBM per device.

```python
import math
import jax
import jax.numpy as jnp
from jax import lax

B = 128
R = 14
KB_DEV = 2
K = 512


def levels(rng, dims, split, low, high):
    def one(axis_at, parts):
        heights = jax.random.uniform(jax.random.fold_in(jax.random.fold_in(rng, 6), axis_at), (parts,), jnp.float32, low / len(split), high / len(split))
        return jnp.repeat(jnp.exp(heights), dims[axis_at] // parts).reshape((-1,) + (1,) * (len(dims) - axis_at - 1))

    level = one(*split[0])
    for cut in split[1:]:
        level = level * one(*cut)
    return level


def centred(own_key, dims, deviation, most, cuts=(), held_as=jnp.bfloat16):
    level = levels(own_key, dims, cuts, -0.22, 0.18) if cuts else 1.0
    array = jax.random.normal(own_key, dims, jnp.float32) * deviation * level
    return jnp.minimum(jnp.maximum(array, -most), most).astype(held_as)


def setup_inputs(seed: int = 0) -> dict:
    keys = jax.random.split(jax.random.key(seed), 13)
    top_rows = centred(keys[0], (R * B, K * B), (K * B) ** -0.5, 0.0234375, ((1, 256),), jnp.float32)
    lower_new = centred(keys[1], (K * B, 2 * B), 1.0, 6.0, ((0, 256),), jnp.float32)
    block_order = jax.vmap(lambda own: jax.random.permutation(own, KB_DEV))(jax.random.split(keys[2], (K // KB_DEV))).reshape((K // KB_DEV, KB_DEV)).astype(jnp.int32)
    corner = centred(keys[3], (R * B, R * B), (R * B) ** -0.5, 0.125, ((0, 2),), jnp.float32)
    target = centred(keys[4], (R * B, 2 * B), 1.0, 6.0, ((0, 2),), jnp.float32)
    coupling = centred(keys[5], (B, B), B ** -0.5, 0.5, (), jnp.float32)
    top_right = centred(keys[6], (R, B, B), B ** -0.5, 0.5, ((0, 2),), jnp.float32)
    top_left = centred(keys[7], (R, B, B), B ** -0.5, 0.5, ((0, 2),), jnp.float32)
    top_values = jnp.clip(jnp.exp(math.log(2.0) - 1.3862944 * jax.random.uniform(keys[8], (R, B), jnp.float32) ** levels(keys[8], (R, B), ((0, 2),), -0.2, 0.2)), 0.5, 2.0)
    new_right = centred(keys[9], (2, B, B), B ** -0.5, 0.5, (), jnp.float32)
    new_left = centred(keys[10], (2, B, B), B ** -0.5, 0.5, (), jnp.float32)
    new_values = jnp.clip(jnp.exp(jax.random.uniform(keys[11], (2, B), jnp.float32, math.log(0.5), math.log(2.0))), 0.5, 2.0)
    return {"top_rows": top_rows, "lower_new": lower_new, "block_order": block_order, "corner": corner, "target": target, "coupling": coupling, "top_right": top_right, "top_left": top_left, "top_values": top_values, "new_right": new_right, "new_left": new_left, "new_values": new_values}


PRECISION = lax.Precision.HIGHEST


def solve_block(right_side, left_right, left_left, left_values, col_right, col_left, col_values):
    rotated = jnp.dot(jnp.dot(left_left, right_side, precision=PRECISION), col_right, precision=PRECISION)
    rotated = rotated / (left_values[:, None] + col_values[None, :])
    return jnp.dot(jnp.dot(left_right, rotated, precision=PRECISION), col_left, precision=PRECISION)


def reference(top_rows, lower_new, block_order, corner, target, coupling, top_right, top_left, top_values, new_right, new_left, new_values):
    groups = K // KB_DEV
    lower_blocks = lower_new.reshape(groups, KB_DEV, B, 2 * B)
    paired = jnp.take_along_axis(lower_blocks, block_order[:, :, None, None].astype(jnp.int32), axis=1).reshape(K * B, 2 * B)
    right_side = target - jnp.dot(top_rows, paired, precision=PRECISION)
    row_block = jnp.arange(R * B) // B
    upper_part = jnp.where(row_block[:, None] < row_block[None, :], corner, jnp.zeros_like(corner))
    solved = [None] * R
    for position in range(R - 1, -1, -1):
        offset = position * B
        left_column = solve_block(right_side[offset:offset + B, :B], top_right[position], top_left[position], top_values[position], new_right[0], new_left[0], new_values[0])
        second_side = right_side[offset:offset + B, B:] - jnp.dot(left_column, coupling, precision=PRECISION)
        right_column = solve_block(second_side, top_right[position], top_left[position], top_values[position], new_right[1], new_left[1], new_values[1])
        combined = jnp.concatenate([left_column, right_column], axis=1)
        right_side = right_side - jnp.dot(upper_part[:, offset:offset + B], combined, precision=PRECISION)
        solved[position] = combined
    return jnp.concatenate(solved, axis=0)
```

```python
import jax
import jax.numpy as jnp
from jax import lax
from jax.experimental import pallas as pl
from jax.experimental.pallas import tpu as pltpu
from jax.sharding import Mesh
from jax.sharding import PartitionSpec as P

COL_ROW = ("col_0", "col_1", "col_2", "row")
B = 128
H = 7
F32 = jnp.float32
BF16 = jnp.bfloat16
MESH = pl.DeviceIdType.MESH
FIRST = ("col_1", "col_0")
SECOND = ("col_0", "col_1")
GROUPS = ((4, 3), (2, 2), (0, 2))


def split(x):
    high = x.astype(BF16)
    return high, (x - high.astype(F32)).astype(BF16)


def mm(a, b):
    return jnp.dot(a, b, preferred_element_type=F32)


def cat(x):
    return jnp.concatenate(split(x), axis=1)


def twice(x):
    return jnp.concatenate([x, x], axis=0)


def dot_left(a_cat, b):
    high, low = split(b)
    return mm(a_cat, twice(high)) + mm(a_cat[:, :B], low)


def dot_right(a, high_twice, low):
    a_high, a_low = split(a)
    return mm(jnp.concatenate([a_high, a_low], axis=1), high_twice) + mm(a_high, low)


def dot3(a, b):
    high, low = split(b)
    return dot_right(a, twice(high), low)


class Links:
    def __init__(self, send, recv):
        self.send, self.recv, self.used, self.pending = send, recv, 0, []

    def slots(self, count):
        first = self.used
        self.used += count
        return first

    def copy(self, src, dst, slot, to):
        return pltpu.make_async_remote_copy(
            src_ref=src,
            dst_ref=dst,
            send_sem=self.send.at[slot],
            recv_sem=self.recv.at[slot],
            device_id=to,
            device_id_type=MESH,
        )


N_SLOTS = 3 + 1 + 18 + 18 + 7 + 7 + 42 + 42 + 14
N_LOCAL = 16


def kernel(
    top_hbm,
    lower_hbm,
    order_ref,
    corner_hbm,
    target_hbm,
    coupling_hbm,
    tr_hbm,
    tl_hbm,
    tv_hbm,
    nr_hbm,
    nl_hbm,
    nv_hbm,
    out_hbm,
    top_far,
    top_own,
    lower,
    u_own,
    u_cross,
    target,
    coupling,
    tr,
    tl,
    tv,
    nr,
    nl,
    nv,
    tr_far,
    xsend,
    xrecv,
    part,
    r1,
    p2,
    r2,
    p3,
    r3,
    g2,
    g1,
    full,
    tn,
    rd,
    tl_cat,
    tr_cat,
    a_buf,
    v_own,
    v_cross,
    upd,
    zs,
    zr,
    ob,
    local_sem,
    send_sem,
    recv_sem,
):
    row = lax.axis_index("row")
    me = {name: lax.axis_index(name) for name in ("col_0", "col_1", "col_2")}
    size = {name: lax.axis_size(name) for name in ("col_0", "col_1", "col_2")}
    n_z = size["col_2"]
    z = me["col_2"]
    other = {"row": 1 - row}
    half = H * B

    def peer(axis, distance):
        return lax.rem(me[axis] + distance, size[axis])

    barrier = pltpu.get_barrier_semaphore()
    pl.semaphore_signal(barrier, inc=1, device_id=other, device_id_type=MESH)
    n_peers = 1
    for axis in ("col_0", "col_1", "col_2"):
        for distance in range(1, size[axis]):
            pl.semaphore_signal(
                barrier, inc=1, device_id={axis: peer(axis, distance)}, device_id_type=MESH
            )
            n_peers += 1

    far_rows = pl.ds(pl.multiple_of((1 - row) * half, B), half)
    own_rows = pl.ds(pl.multiple_of(row * half, B), half)
    loads = [
        (lower_hbm, lower),
        (nr_hbm, nr),
        (top_hbm.at[far_rows], top_far),
        (top_hbm.at[own_rows], top_own),
        (tr_hbm, tr),
        (nl_hbm, nl),
        (coupling_hbm, coupling),
        (nv_hbm, nv),
        (tv_hbm, tv),
        (target_hbm, target),
        (tl_hbm, tl),
        (corner_hbm.at[:, own_rows], u_own),
        (corner_hbm.at[:, pl.ds(half, half)], u_cross),
    ]
    loads = [
        pltpu.make_async_copy(src, dst, local_sem.at[i]) for i, (src, dst) in enumerate(loads)
    ]
    for load in loads:
        load.start()

    links = Links(send_sem, recv_sem)
    sent = []

    loads[0].wait()
    loads[1].wait()
    paired = [
        jnp.where(order_ref[0, p] == 0, lower[0:B], lower[B : 2 * B]) for p in range(2)
    ]
    nr_split = [split(nr[c]) for c in range(2)]
    rotated = [
        jnp.concatenate(
            [
                dot_right(paired[p][:, c * B : (c + 1) * B], twice(nr_split[c][0]), nr_split[c][1])
                for c in range(2)
            ],
            axis=1,
        )
        for p in range(2)
    ]
    pair_high, pair_low = split(jnp.concatenate(rotated, axis=0))

    def partial(rows_ref, first, count, dst):
        for j in range(first, first + count):
            a_high, a_low = split(rows_ref[j * B : (j + 1) * B])
            value = mm(a_high, pair_high) + mm(a_low, pair_high) + mm(a_high, pair_low)
            for c in range(2):
                dst[c, j] = value[:, c * B : (c + 1) * B].reshape(4, 32, B)

    loads[2].wait()
    exchange_slot = links.slots(len(GROUPS))
    exchanges = []
    for g, (first, count) in enumerate(GROUPS):
        partial(top_far, first, count, xsend)
        if g == 0:
            pl.semaphore_wait(barrier, n_peers)
        window = pl.ds(first, count)
        exchange = links.copy(
            xsend.at[:, window], xrecv.at[:, window], exchange_slot + g, other
        )
        exchange.start()
        exchanges.append(exchange)
        sent.append(exchange)
    loads[3].wait()
    for g, (first, count) in enumerate(GROUPS):
        partial(top_own, first, count, part)

    slot_r1 = links.slots(2 * 3 * len(GROUPS))
    copies_r1 = {}
    for g, (first, count) in enumerate(GROUPS):
        window = pl.ds(first, count)
        exchanges[g].wait_recv()
        part[:, first : first + count] += xrecv[:, first : first + count]
        for distance in (2, 1, 3):
            for c in range(2):
                to = peer(FIRST[c], distance)
                copy = links.copy(
                    part.at[c, window, to],
                    r1.at[c, distance - 1, window],
                    slot_r1 + (g * 3 + distance - 1) * 2 + c,
                    {FIRST[c]: to},
                )
                copy.start()
                copies_r1[g, c, distance] = copy
                sent.append(copy)

    loads[4].wait()
    slot_tr = links.slots(1)
    swap = links.copy(tr, tr_far, slot_tr, other)
    swap.start()
    sent.append(swap)

    for load in loads[5:]:
        load.wait()
    nl_split = [split(nl[c]) for c in range(2)]
    m0 = dot_right(nl[0], twice(nr_split[0][0]), nr_split[0][1])
    m1 = dot_right(nl[1], twice(nr_split[1][0]), nr_split[1][1])
    pc = dot_right(dot3(nl[0], coupling[...]), twice(nr_split[1][0]), nr_split[1][1])
    rhs0 = split(jnp.concatenate([m0, pc, nl[0]], axis=1))
    rhs1 = split(jnp.concatenate([m1, nl[1]], axis=1))
    for j in range(H):
        tl_cat[j] = cat(tl[j])
        tr_cat[j] = cat(tr[j])
        column = jnp.broadcast_to(tv[j : j + 1], (B, B)).T
        for c in range(2):
            rd[c, j] = 1.0 / (column + nv[c : c + 1])
            tn[c, j] = dot_right(
                target[j * B : (j + 1) * B, c * B : (c + 1) * B],
                twice(nr_split[c][0]),
                nr_split[c][1],
            )
            upd[c, j] = jnp.zeros((B, B), F32)

    def rotate_blocks(u_ref, right_of, v_ref):
        def left(i, carry):
            rows = pl.ds(pl.multiple_of(i * B, B), B)
            value = dot_left(tl_cat[i], u_ref[rows, :])
            for k in range(H):
                a_buf[k, rows] = value[:, k * B : (k + 1) * B]
            return carry

        lax.fori_loop(0, H, left, 0)

        def right(k, carry):
            high, low = split(right_of[k])
            value = dot_right(a_buf[k], twice(high), low)
            v_ref[k] = cat(value)
            return carry

        lax.fori_loop(0, H, right, 0)

    rotate_blocks(u_own, tr, v_own)
    for j in range(H):
        v_own[j, j * B : (j + 1) * B] = cat(dot_left(tl_cat[j], tr[j]))

    swap.wait_recv()

    @pl.when(row == 0)
    def _():
        rotate_blocks(u_cross, tr_far, v_cross)

    slot_r2 = links.slots(2 * 3 * len(GROUPS))
    copies_r2 = {}
    for g, (first, count) in enumerate(GROUPS):
        window = pl.ds(first, count)
        for c in range(2):
            for distance in (1, 2, 3):
                copies_r1[g, c, distance].wait_recv()
            mine = me[FIRST[c]]
            value = part[c, window, mine]
            for distance in (1, 2, 3):
                value = value + r1[c, distance - 1, window]
            p2[c, window] = value.reshape(count, 4, 8, B)
        for distance in (2, 1, 3):
            for c in range(2):
                to = peer(SECOND[c], distance)
                copy = links.copy(
                    p2.at[c, window, to],
                    r2.at[c, distance - 1, window],
                    slot_r2 + (g * 3 + distance - 1) * 2 + c,
                    {SECOND[c]: to},
                )
                copy.start()
                copies_r2[g, c, distance] = copy
                sent.append(copy)

    for g, (first, count) in enumerate(GROUPS):
        window = pl.ds(first, count)
        for c in range(2):
            for distance in (1, 2, 3):
                copies_r2[g, c, distance].wait_recv()
            mine = me[SECOND[c]]
            value = p2[c, window, mine]
            for distance in (1, 2, 3):
                value = value + r2[c, distance - 1, window]
            p3[window, c] = value
    slot_r3 = links.slots(n_z - 1)
    slot_g3 = links.slots(n_z - 1)
    far_first = sorted(range(1, n_z), key=lambda d: -min(d, n_z - d))

    def down(distance):
        to = peer("col_2", distance)
        return to, links.copy(
            p3.at[to], r3.at[distance - 1], slot_r3 + distance - 1, {"col_2": to}
        )

    for distance in far_first:
        to, copy = down(distance)

        @pl.when(to < H)
        def _():
            copy.start()

    def up_copy(distance):
        return pltpu.make_async_remote_copy(
            src_ref=g2.at[z],
            dst_ref=g2.at[z],
            send_sem=send_sem.at[slot_g3 + distance - 1],
            recv_sem=recv_sem.at[slot_g3 + z],
            device_id={"col_2": peer("col_2", distance)},
            device_id_type=MESH,
        )

    @pl.when(z < H)
    def _():
        value = p3[z]
        for distance in range(1, n_z):
            down(distance)[1].wait_recv()
        for distance in range(1, n_z):
            value = value + r3[distance - 1]
        g2[z] = value
        for distance in far_first:
            up_copy(distance).start()

    slot_g2 = links.slots(2 * 3 * H)
    slot_g1 = links.slots(2 * 3 * H)
    copies_g1 = {}

    def arrival(j):
        return pltpu.make_async_remote_copy(
            src_ref=g2.at[j],
            dst_ref=g2.at[j],
            send_sem=send_sem.at[slot_g3],
            recv_sem=recv_sem.at[slot_g3 + j],
            device_id={"col_2": peer("col_2", 1)},
            device_id_type=MESH,
        )

    def second_copy(j, c, distance):
        mine = me[SECOND[c]]
        return links.copy(
            g2.at[j, c],
            g1.at[c, j, mine],
            slot_g2 + (j * 3 + distance - 1) * 2 + c,
            {SECOND[c]: peer(SECOND[c], distance)},
        )

    def first_copy(j, c, distance):
        mine = me[FIRST[c]]
        return links.copy(
            g1.at[c, j],
            full.at[c, j, mine],
            slot_g1 + (j * 3 + distance - 1) * 2 + c,
            {FIRST[c]: peer(FIRST[c], distance)},
        )

    for j in range(H - 1, -1, -1):

        @pl.when(z != j)
        def _():
            arrival(j).wait_recv()

        for distance in (2, 1, 3):
            for c in range(2):
                copy = second_copy(j, c, distance)
                copy.start()
                sent.append(copy)
        for c in range(2):
            g1[c, j, me[SECOND[c]]] = g2[j, c]
    for j in range(H - 1, -1, -1):
        for c in range(2):
            for distance in (1, 2, 3):
                second_copy(j, c, distance).wait_recv()
        for distance in (2, 1, 3):
            for c in range(2):
                copy = first_copy(j, c, distance)
                copy.start()
                sent.append(copy)
        for c in range(2):
            full[c, j, me[FIRST[c]]] = g1[c, j]

    slot_z = links.slots(2 * H)

    def z_copy(k, c):
        return links.copy(zs.at[c, k], zr.at[c, k], slot_z + k * 2 + c, other)

    @pl.when(row == 0)
    def _():
        for k in range(H - 1, -1, -1):
            for c in range(2):
                z_copy(k, c).wait_recv()
            high, low = split(jnp.concatenate([zr[0, k], zr[1, k]], axis=1))
            value = mm(v_cross[k], twice(high)) + mm(v_cross[k, :, :B], low)
            for c in range(2):
                upd[c] += value[:, c * B : (c + 1) * B].reshape(H, B, B)

    def block_rows(i):
        return slice(i * B, (i + 1) * B)

    rhs0 = (twice(rhs0[0]), rhs0[1])
    rhs1 = (twice(rhs1[0]), rhs1[1])
    before = {}
    for step in range(H + 1):
        b0, b1 = H - 1 - step, H - step
        new = {}
        if b0 >= 0:
            for distance in (1, 2, 3):
                first_copy(b0, 0, distance).wait_recv()
        if b1 < H:
            for distance in (1, 2, 3):
                first_copy(b1, 1, distance).wait_recv()
        heads = []
        if b0 >= 0:
            side = tn[0, b0] - full[0, b0].reshape(B, B)
            value = dot_left(tl_cat[b0], side) - upd[0, b0]
            if step > 0:
                value = value - dot_left(v_own[b0 + 1, block_rows(b0)], before["z0"])
            core = value * rd[0, b0]
            heads = dot_right(core, *rhs0)
            new["z0"] = heads[:, :B]
            new["q"] = heads[:, B : 2 * B]
            new["y0"] = heads[:, 2 * B :]
            zs[0, b0] = new["z0"]
        if b1 < H:
            side = tn[1, b1] - full[1, b1].reshape(B, B)
            value = dot_left(tl_cat[b1], side) - upd[1, b1]
            value = value - dot_left(v_own[b1, block_rows(b1)], before["q"])
            if step > 1:
                value = value - dot_left(v_own[b1 + 1, block_rows(b1)], before["z1"])
            core = value * rd[1, b1]
            heads = dot_right(core, *rhs1)
            new["z1"] = heads[:, :B]
            new["y1"] = heads[:, B:]
            zs[1, b1] = new["z1"]

        @pl.when(row == 1)
        def _():
            if b0 >= 0:
                z_copy(b0, 0).start()
            if b1 < H:
                z_copy(b1, 1).start()

        if step > 0 and b0 > 0:
            value = dot_left(v_own[b0 + 1, : b0 * B], before["z0"])
            upd[0, :b0] += value.reshape(b0, B, B)
        if step > 1 and b1 > 0:
            value = dot_left(v_own[b1 + 1, : b1 * B], before["z1"])
            upd[1, :b1] += value.reshape(b1, B, B)
        if b0 >= 0:
            ob[block_rows(b0), :B] = dot_left(tr_cat[b0], new["y0"])
        if b1 < H:
            ob[block_rows(b1), B:] = dot_left(tr_cat[b1], new["y1"])
        before = new

    store = pltpu.make_async_copy(ob, out_hbm, local_sem.at[N_LOCAL - 1])
    store.start()
    for copy in sent:
        copy.wait_send()
    for distance in far_first:
        to, copy = down(distance)

        @pl.when(to < H)
        def _():
            copy.wait_send()

    @pl.when(z < H)
    def _():
        for distance in far_first:
            up_copy(distance).wait_send()

    @pl.when(row == 1)
    def _():
        for k in range(H):
            for c in range(2):
                z_copy(k, c).wait_send()

    store.wait()


def shards(*args):
    any_space = pl.BlockSpec(memory_space=pl.ANY)
    specs = [any_space] * 12
    specs[2] = pl.BlockSpec(memory_space=pltpu.SMEM)
    half = H * B

    def buffer(*lengths, dtype=F32):
        return pltpu.VMEM(lengths, dtype)

    scratch = [
        buffer(half, 2 * B),
        buffer(half, 2 * B),
        buffer(2 * B, 2 * B),
        buffer(half, half),
        buffer(half, half),
        buffer(half, 2 * B),
        buffer(B, B),
        buffer(H, B, B),
        buffer(H, B, B),
        buffer(H, B),
        buffer(2, B, B),
        buffer(2, B, B),
        buffer(2, B),
        buffer(H, B, B),
        buffer(2, H, 4, 32, B),
        buffer(2, H, 4, 32, B),
        buffer(2, H, 4, 32, B),
        buffer(2, 3, H, 32, B),
        buffer(2, H, 4, 8, B),
        buffer(2, 3, H, 8, B),
        buffer(H + 1, 2, 8, B),
        buffer(7, 2, 8, B),
        buffer(H + 1, 2, 8, B),
        buffer(2, H, 4, 8, B),
        buffer(2, H, 4, 4, 8, B),
        buffer(2, H, B, B),
        buffer(2, H, B, B),
        buffer(H, B, 2 * B, dtype=BF16),
        buffer(H, B, 2 * B, dtype=BF16),
        buffer(H, half, B),
        buffer(H, half, 2 * B, dtype=BF16),
        buffer(H, half, 2 * B, dtype=BF16),
        buffer(2, H, B, B),
        buffer(2, H, B, B),
        buffer(2, H, B, B),
        buffer(half, 2 * B),
        pltpu.SemaphoreType.DMA((N_LOCAL,)),
        pltpu.SemaphoreType.DMA((N_SLOTS,)),
        pltpu.SemaphoreType.DMA((N_SLOTS,)),
    ]
    return pl.pallas_call(
        kernel,
        out_shape=jax.ShapeDtypeStruct((half, 2 * B), F32),
        in_specs=specs,
        out_specs=any_space,
        scratch_shapes=scratch,
        compiler_params=pltpu.CompilerParams(collective_id=0, has_side_effects=True),
    )(*args)


def solution(mesh):
    torus = Mesh(
        mesh.devices.reshape(4, 4, 8, mesh.shape["row"]), ("col_0", "col_1", "col_2", "row")
    )
    in_specs = (
        P(None, COL_ROW),
        P(COL_ROW, None),
        P(COL_ROW, None),
        P("row", None),
        P("row", None),
        P(),
        P("row", None, None),
        P("row", None, None),
        P("row", None),
        P(),
        P(),
        P(),
    )
    out_specs = P("row", None)
    return jax.shard_map(
        shards, mesh=torus, in_specs=in_specs, out_specs=out_specs, check_vma=False
    )
```
